32 devices in a mesh: cols: 8 (over z, x), trc: 4 (over y, core).
Axes of the slice: x: 2, y: 2, z: 4, core: 2. Of those that a mesh axis runs over, the one named last changes fastest.
Arguments:
- tracers_src: bfloat16 [28, 127, 16384], P(None, None, ('cols', 'trc')), may hold values from -1 to 2
- layer_dp: float32 [127, 16384], P(None, ('cols', 'trc')), may hold values from 0.3 to 3
- cut_frac: float32 [71, 16384], P(None, ('cols', 'trc')), may hold values from 0.05 to 0.95
- level_bounds: int32 [2, 72, 16384], P(None, None, ('cols', 'trc')), may hold values from 0 to 126, as said below
Outputs:
- remapped_tracers: bfloat16 [28, 72, 16384], P('trc', None, 'cols')
- burden: float32 [28], P('trc')
The draws below stay inside these ranges and needn't reach their ends.
Inputs may be any that keep to these rules, and one draw needn't show every extreme that they name: level_bounds[0, 0, c] = 0, level_bounds[1, 71, c] = 126, level_bounds[1, t, c] = level_bounds[0, t + 1, c], and level_bounds[0, t, c] rises strictly with t in every column.
All inputs are finite; a program needn't handle non-finite values.
Results may differ from the reference program's by a relative error of at most 0.0005.
Values may be sent and summed in bfloat16 or wider, within the bound.
A program may use at most 64 MiB of HBM per device.

```python
import math
import jax
import jax.numpy as jnp
from jax import lax

TR = 28
KS = 127
KT = 72
COLS = 16384


def draw_level_bounds(key, part):
    random_scores = jax.random.randint(key, (KS - 2, COLS), 0, 1 << 20)
    random_scores = random_scores * (KS - 2) + lax.broadcasted_iota(jnp.int32, (KS - 2, COLS), 0)
    ordering = jnp.argsort(random_scores, axis=0)
    picked = jnp.sort(ordering[:KT - 1], axis=0).astype(jnp.int32) + 1
    first_layer = jnp.concatenate([jnp.zeros((1, COLS), jnp.int32), picked], axis=0)
    last_layer = jnp.concatenate([picked, jnp.full((1, COLS), KS - 1, jnp.int32)], axis=0)
    return jnp.stack([first_layer, last_layer]).astype(jnp.int32)


def levels(rng, extent, pieces, least, high):
    gain, own = 1.0, jax.random.fold_in(rng, 6)
    for dim, shards_of in pieces:
        heights = jnp.exp(jax.random.uniform(jax.random.fold_in(own, dim), (shards_of,), jnp.float32, least / len(pieces), high / len(pieces)))
        gain = gain * jnp.repeat(heights, extent[dim] // shards_of).reshape([-1 if axis == dim else 1 for axis in range(len(extent))])
    return gain


def setup_inputs(seed: int = 0) -> dict:
    streams_of = jax.random.split(jax.random.key(seed), 5)
    tracers_src = jnp.clip(-1.0 + 3.0 * jax.random.uniform(streams_of[0], (TR, KS, COLS), jnp.float32) ** levels(streams_of[0], (TR, KS, COLS), ((2, 32),), -0.2, 0.2), -1.0, 2.0).astype(jnp.bfloat16)
    layer_dp = jnp.clip(jnp.exp(math.log(3.0) - 2.3025851 * jax.random.uniform(streams_of[1], (KS, COLS), jnp.float32) ** levels(streams_of[1], (KS, COLS), ((1, 32),), -0.2, 0.2)), 0.3, 3.0)
    cut_frac = jnp.clip(0.05 + 0.9 * jax.random.uniform(streams_of[2], (KT - 1, COLS), jnp.float32) ** levels(streams_of[2], (KT - 1, COLS), ((1, 32),), -0.2, 0.2), 0.05, 0.95)
    level_bounds = draw_level_bounds(jax.random.fold_in(streams_of[4], 71), 0)
    return {"tracers_src": tracers_src, "layer_dp": layer_dp, "cut_frac": cut_frac, "level_bounds": level_bounds}


def remap_block(tracers, layer_dp, cut_frac, bounds):
    columns = layer_dp.shape[1]
    tracer_count = tracers.shape[0]
    src_edges = jnp.concatenate([jnp.zeros((1, columns), jnp.float32), jnp.cumsum(layer_dp, axis=0)], axis=0)
    inner_first = bounds[0][1:].astype(jnp.int32)
    base_edge = jnp.take_along_axis(src_edges, inner_first, axis=0)
    chosen_dp = jnp.take_along_axis(layer_dp, inner_first, axis=0)
    inner_edges = base_edge + cut_frac * chosen_dp
    targets = jnp.concatenate([jnp.zeros((1, columns), jnp.float32), inner_edges, src_edges[-1:]], axis=0)
    layer_mass = tracers.astype(jnp.float32) * layer_dp[None]
    cum_mass = jnp.concatenate([jnp.zeros((tracer_count, 1, columns), jnp.float32), jnp.cumsum(layer_mass, axis=1)], axis=1)
    index_all = jnp.broadcast_to(inner_first[None], (tracer_count,) + inner_first.shape)
    inner_mass = jnp.take_along_axis(cum_mass, index_all, axis=1) + cut_frac[None] * jnp.take_along_axis(layer_mass, index_all, axis=1)
    edge_mass = jnp.concatenate([jnp.zeros((tracer_count, 1, columns), jnp.float32), inner_mass, cum_mass[:, -1:]], axis=1)
    remapped = edge_mass[:, 1:] - edge_mass[:, :-1]
    return remapped, targets[1:] - targets[:-1], cum_mass[:, -1]


def reference(tracers_src, layer_dp, cut_frac, level_bounds):
    block_cols = math.gcd(COLS, 512)
    block_count = COLS // block_cols

    def remap_one(block_index):
        offset = block_index * block_cols
        return remap_block(
            lax.dynamic_slice_in_dim(tracers_src, offset, block_cols, 2),
            lax.dynamic_slice_in_dim(layer_dp, offset, block_cols, 1),
            lax.dynamic_slice_in_dim(cut_frac, offset, block_cols, 1),
            lax.dynamic_slice_in_dim(level_bounds, offset, block_cols, 2))

    remapped, target_dp, column_mass = lax.map(remap_one, jnp.arange(block_count, dtype=jnp.int32))
    remapped = jnp.moveaxis(remapped, 0, 2).reshape(TR, KT, COLS)
    target_dp = jnp.moveaxis(target_dp, 0, 1).reshape(KT, COLS)
    column_mass = jnp.moveaxis(column_mass, 0, 1).reshape(TR, COLS)
    position = lax.broadcasted_iota(jnp.int32, (COLS,), 0)
    cell_area = 1.0 + 2.0 * position.astype(jnp.float32) / COLS
    norm_scale = 1.0 / (COLS * KS)
    burden = jnp.sum(column_mass * cell_area[None], axis=1) * norm_scale
    positive = jnp.maximum(remapped / target_dp[None], 0.0)
    burden_after = jnp.sum(positive * target_dp[None] * cell_area[None, None], axis=(1, 2)) * norm_scale
    fix_ratio = burden / burden_after
    return (positive * fix_ratio[:, None, None]).astype(jnp.bfloat16), burden
```

```python
import functools

import jax
import jax.numpy as jnp
from jax import lax
from jax.experimental import pallas as pl
from jax.experimental.pallas import tpu as pltpu
from jax.sharding import PartitionSpec as P

MESH = pl.DeviceIdType.MESH
F32 = jnp.float32
LANES = 128
ROWS = 8


def take_rows(values, rows):
    return jnp.take_along_axis(values, rows, axis=0, mode="promise_in_bounds")


def running_sum(pieces, row):
    result, carry = [], None
    last = jnp.full((ROWS, LANES), ROWS - 1, jnp.int32)
    for piece in pieces:
        for step in (1, 2, 4):
            piece = piece + jnp.where(row >= step, pltpu.roll(piece, step, 0), 0.0)
        total = take_rows(piece, last)
        result.append(piece if carry is None else piece + carry)
        carry = total if carry is None else carry + total
    return result


def edge_values(values, low, high, layers, levels):
    slack = layers - levels
    edges = []
    for piece in range(levels // ROWS):
        first = (piece * ROWS + 1) // ROWS
        final = min((piece * ROWS + ROWS + slack) // ROWS, len(values) - 1)
        picked = None
        for source in range(first, final + 1):
            here = take_rows(values[source], low[piece])
            picked = here if picked is None else jnp.where(high[piece] == source, here, picked)
        edges.append(picked)
    return edges


def differences(edges, row):
    result, before = [], jnp.zeros((ROWS, LANES), F32)
    for edge in edges:
        turned = pltpu.roll(edge, 1, 0)
        result.append(edge - jnp.where(row == 0, before, turned))
        before = turned
    return result


def kernel(
    cols, groups, x_ref, dp_ref, cut_ref, bounds_ref, out_ref, burden_ref,
    positive, stage, mass_rows, dp_rows, blend, target, inverse, part, packed, arrived, ratio,
    sum_send, sum_recv, move_send, move_recv, own_sem,
):
    tracers, layers, columns = x_ref.shape
    levels = bounds_ref.shape[1]
    per = tracers // groups
    devices = cols * groups
    pieces = (layers + ROWS) // ROWS
    slack = layers - levels
    c_id, g_id = lax.axis_index("cols"), lax.axis_index("trc")
    me = c_id * groups + g_id
    norm = 1.0 / (columns * devices * layers)

    barrier = pltpu.get_barrier_semaphore()
    for step in range(1, devices):
        peer = lax.rem(me + step, devices)
        pl.semaphore_signal(
            barrier, inc=1, device_id=(peer // groups, lax.rem(peer, groups)), device_id_type=MESH
        )

    row = lax.broadcasted_iota(jnp.int32, (ROWS, LANES), 0)
    lane = lax.broadcasted_iota(jnp.int32, (1, LANES), 1)
    part[...] = jnp.zeros_like(part)
    mass_rows[...] = jnp.zeros_like(mass_rows)
    dp_rows[...] = jnp.zeros_like(dp_rows)

    def column_block(block, _):
        offset = pl.multiple_of(block * LANES, LANES)
        cs = pl.ds(offset, LANES)
        target[0 : levels - 1] = bounds_ref[0, 1:, cs]
        target[levels - 1 : levels] = jnp.full((1, LANES), layers, jnp.int32)
        dp_rows[0:layers] = dp_ref[:, cs]
        for piece in range(pieces):
            first = max(1, piece * ROWS - slack)
            final = min(levels - 1, piece * ROWS + ROWS - 1)
            weight = jnp.full((ROWS, LANES), -1.0, F32)
            for j in range(first, final + 1):
                found = target[j - 1 : j] == row + piece * ROWS
                weight = jnp.where(found, cut_ref[j - 1 : j, cs] - 1.0, weight)
            blend[piece] = weight
        bounds = [target[p * ROWS : (p + 1) * ROWS] for p in range(levels // ROWS)]
        low = [jnp.bitwise_and(b, ROWS - 1) for b in bounds]
        high = [lax.shift_right_logical(b, 3) for b in bounds]

        def remap(mass):
            sums = running_sum(mass, row)
            values = [s + blend[p] * m for p, (s, m) in enumerate(zip(sums, mass))]
            edges = edge_values(values, low, high, layers, levels)
            return differences(edges, row), values[-1]

        thickness, _ = remap([dp_rows[p * ROWS : (p + 1) * ROWS] for p in range(pieces)])
        for p, t in enumerate(thickness):
            inverse[p] = 1.0 / t
        area = 1.0 + 2.0 * (lane + offset + me * columns).astype(F32) / (columns * devices)

        def tracer(q, _):
            mass_rows[0:layers] = x_ref[q, :, cs].astype(F32)
            mass = [
                mass_rows[p * ROWS : (p + 1) * ROWS] * dp_rows[p * ROWS : (p + 1) * ROWS]
                for p in range(pieces)
            ]
            moved, top = remap(mass)
            kept = jnp.zeros((ROWS, LANES), F32)
            for p, m in enumerate(moved):
                m = jnp.maximum(m, 0.0)
                kept = kept + m
                positive[q, p * ROWS : (p + 1) * ROWS, cs] = m * inverse[p]
            before = top[layers % ROWS : layers % ROWS + 1]
            part[0, pl.ds(q, 1), :] += before * area
            part[1, pl.ds(q, 1), :] += jnp.sum(kept, axis=0, keepdims=True) * area
            return 0

        return lax.fori_loop(0, tracers, tracer, 0)

    lax.fori_loop(0, columns // LANES, column_block, 0)

    t_row = lax.broadcasted_iota(jnp.int32, (tracers, LANES), 0)
    t_lane = lax.broadcasted_iota(jnp.int32, (tracers, LANES), 1)

    def to_row(values, shift):
        return jnp.sum(jnp.where(t_row == t_lane + shift, values, 0.0), axis=0, keepdims=True)

    def to_column(values):
        return jnp.sum(jnp.where(t_row == t_lane, values, 0.0), axis=1, keepdims=True)

    packed[...] = jnp.zeros_like(packed)
    for kind in range(2):
        packed[kind : kind + 1] = to_row(jnp.sum(part[kind], axis=1, keepdims=True), 0)
    arrived[pl.ds(me, 1)] = packed[...][None]
    pl.semaphore_wait(barrier, devices - 1)
    sums = []
    for step in range(1, devices):
        peer = lax.rem(me + step, devices)
        copy = pltpu.make_async_remote_copy(
            src_ref=packed, dst_ref=arrived.at[me], send_sem=sum_send.at[step - 1], recv_sem=sum_recv.at[step - 1],
            device_id=(peer // groups, lax.rem(peer, groups)), device_id_type=MESH,
        )
        copy.start()
        sums.append(copy)
    for copy in sums:
        copy.wait()
    total = jnp.sum(arrived[...], axis=0) * norm
    before = to_column(total[0:1])
    after = to_column(total[1:2])
    ratio[...] = jnp.broadcast_to(before / after, (tracers, LANES))
    burden_ref[...] = to_row(before, g_id * per)[:, 0:per]

    place = pl.ds(pl.multiple_of(g_id * columns, LANES), columns)

    def fill(h, q):
        t = h * per + q
        scale = jnp.tile(ratio[pl.ds(t, 1), :], (1, columns // LANES))
        stage[h, q] = (positive[t] * scale).astype(jnp.bfloat16)

    order = sorted(range(1, groups), reverse=True)
    copies = []
    for q in range(per):
        for k in order:
            h = jnp.bitwise_xor(g_id, k)
            fill(h, q)
            copy = pltpu.make_async_remote_copy(
                src_ref=stage.at[h, q], dst_ref=out_ref.at[q, :, place],
                send_sem=move_send.at[q, k - 1], recv_sem=move_recv.at[q, k - 1],
                device_id=(c_id, h), device_id_type=MESH,
            )
            copy.start()
            copies.append(copy)
    for q in range(per):
        fill(g_id, q)
    own = pltpu.make_async_copy(stage.at[g_id], out_ref.at[:, :, place], own_sem)
    own.start()
    own.wait()
    for copy in copies:
        copy.wait()


def per_device(cols, groups, tracers_src, layer_dp, cut_frac, level_bounds):
    tracers, layers, columns = tracers_src.shape
    levels = level_bounds.shape[1]
    per = tracers // groups
    padded = -(-(layers + 1) // ROWS) * ROWS
    vmem = pl.BlockSpec(memory_space=pltpu.VMEM)
    result, burden = pl.pallas_call(
        functools.partial(kernel, cols, groups),
        out_shape=(
            jax.ShapeDtypeStruct((per, levels, columns * groups), jnp.bfloat16),
            jax.ShapeDtypeStruct((1, per), F32),
        ),
        in_specs=[vmem] * 4,
        out_specs=(pl.BlockSpec(memory_space=pl.ANY), vmem),
        scratch_shapes=[
            pltpu.VMEM((tracers, levels, columns), F32),
            pltpu.VMEM((groups, per, levels, columns), jnp.bfloat16),
            pltpu.VMEM((padded, LANES), F32),
            pltpu.VMEM((padded, LANES), F32),
            pltpu.VMEM((padded // ROWS, ROWS, LANES), F32),
            pltpu.VMEM((levels, LANES), jnp.int32),
            pltpu.VMEM((levels // ROWS, ROWS, LANES), F32),
            pltpu.VMEM((2, tracers, LANES), F32),
            pltpu.VMEM((ROWS, LANES), F32),
            pltpu.VMEM((cols * groups, ROWS, LANES), F32),
            pltpu.VMEM((tracers, LANES), F32),
            pltpu.SemaphoreType.DMA((cols * groups - 1,)),
            pltpu.SemaphoreType.DMA((cols * groups - 1,)),
            pltpu.SemaphoreType.DMA((per, groups - 1)),
            pltpu.SemaphoreType.DMA((per, groups - 1)),
            pltpu.SemaphoreType.DMA,
        ],
        compiler_params=pltpu.CompilerParams(
            collective_id=0, has_side_effects=True, vmem_limit_bytes=60 * 1024 * 1024
        ),
        name="remap_fix_exchange",
    )(tracers_src, layer_dp, cut_frac, level_bounds)
    return result, burden.reshape(per)


def solution(mesh):
    spread = ("cols", "trc")
    in_specs = (P(None, None, spread), P(None, spread), P(None, spread), P(None, None, spread))
    out_specs = (P("trc", None, "cols"), P("trc"))
    return jax.shard_map(
        functools.partial(per_device, mesh.shape["cols"], mesh.shape["trc"]),
        mesh=mesh, in_specs=in_specs, out_specs=out_specs, check_vma=False,
    )
```

```python
import functools

import jax
import jax.numpy as jnp
from jax import lax
from jax.experimental import pallas as pl
from jax.experimental.pallas import tpu as pltpu
from jax.sharding import PartitionSpec as P

MESH = pl.DeviceIdType.MESH
F32 = jnp.float32
LANES = 128
ROWS = 8
EARLY = 2


def take_rows(values, rows):
    return jnp.take_along_axis(values, rows, axis=0, mode="promise_in_bounds")


def running_sum(pieces, row):
    result, carry = [], None
    last = jnp.full((ROWS, LANES), ROWS - 1, jnp.int32)
    for piece in pieces:
        for step in (1, 2, 4):
            piece = piece + jnp.where(row >= step, pltpu.roll(piece, step, 0), 0.0)
        total = take_rows(piece, last)
        result.append(piece if carry is None else piece + carry)
        carry = total if carry is None else carry + total
    return result


def edge_values(values, low, high, layers, levels):
    slack = layers - levels
    edges = []
    for piece in range(levels // ROWS):
        first = (piece * ROWS + 1) // ROWS
        final = min((piece * ROWS + ROWS + slack) // ROWS, len(values) - 1)
        picked = None
        for source in range(first, final + 1):
            here = take_rows(values[source], low[piece])
            picked = here if picked is None else jnp.where(high[piece] == source, here, picked)
        edges.append(picked)
    return edges


def differences(edges, row):
    result, before = [], jnp.zeros((ROWS, LANES), F32)
    for edge in edges:
        turned = pltpu.roll(edge, 1, 0)
        result.append(edge - jnp.where(row == 0, before, turned))
        before = turned
    return result


def kernel(
    cols, groups, x_ref, dp_ref, cut_ref, bounds_ref, out_ref, burden_ref,
    positive, stage, mass_rows, dp_rows, blend, target, inverse, part, packed, arrived, ratio,
    early, landed, sum_send, sum_recv, move_send, move_recv, early_send, early_recv, own_sem,
):
    tracers, layers, columns = x_ref.shape
    levels = bounds_ref.shape[1]
    per = tracers // groups
    devices = cols * groups
    pieces = (layers + ROWS) // ROWS
    slack = layers - levels
    c_id, g_id = lax.axis_index("cols"), lax.axis_index("trc")
    me = c_id * groups + g_id
    norm = 1.0 / (columns * devices * layers)

    barrier = pltpu.get_barrier_semaphore()
    for step in range(1, devices):
        peer = lax.rem(me + step, devices)
        pl.semaphore_signal(
            barrier, inc=1, device_id=(peer // groups, lax.rem(peer, groups)), device_id_type=MESH
        )

    row = lax.broadcasted_iota(jnp.int32, (ROWS, LANES), 0)
    lane = lax.broadcasted_iota(jnp.int32, (1, LANES), 1)
    part[...] = jnp.zeros_like(part)
    mass_rows[...] = jnp.zeros_like(mass_rows)
    dp_rows[...] = jnp.zeros_like(dp_rows)

    order = sorted(range(1, groups), reverse=True)

    def early_copies(block, cs):
        copies = []
        for e in range(EARLY):
            for k in order:
                h = jnp.bitwise_xor(g_id, k)
                copies.append(pltpu.make_async_remote_copy(
                    src_ref=positive.at[h * per + e, :, cs], dst_ref=early.at[k - 1, e, :, cs],
                    send_sem=early_send.at[block, e, k - 1], recv_sem=early_recv.at[block, e, k - 1],
                    device_id=(c_id, h), device_id_type=MESH,
                ))
        return copies

    def column_block(block, _):
        offset = pl.multiple_of(block * LANES, LANES)
        cs = pl.ds(offset, LANES)
        target[0 : levels - 1] = bounds_ref[0, 1:, cs]
        target[levels - 1 : levels] = jnp.full((1, LANES), layers, jnp.int32)
        dp_rows[0:layers] = dp_ref[:, cs]
        for piece in range(pieces):
            first = max(1, piece * ROWS - slack)
            final = min(levels - 1, piece * ROWS + ROWS - 1)
            weight = jnp.full((ROWS, LANES), -1.0, F32)
            for j in range(first, final + 1):
                found = target[j - 1 : j] == row + piece * ROWS
                weight = jnp.where(found, cut_ref[j - 1 : j, cs] - 1.0, weight)
            blend[piece] = weight
        bounds = [target[p * ROWS : (p + 1) * ROWS] for p in range(levels // ROWS)]
        low = [jnp.bitwise_and(b, ROWS - 1) for b in bounds]
        high = [lax.shift_right_logical(b, 3) for b in bounds]

        def remap(mass):
            sums = running_sum(mass, row)
            values = [s + blend[p] * m for p, (s, m) in enumerate(zip(sums, mass))]
            edges = edge_values(values, low, high, layers, levels)
            return differences(edges, row), values[-1]

        thickness, _ = remap([dp_rows[p * ROWS : (p + 1) * ROWS] for p in range(pieces)])
        for p, t in enumerate(thickness):
            inverse[p] = 1.0 / t
        area = 1.0 + 2.0 * (lane + offset + me * columns).astype(F32) / (columns * devices)

        def tracer(step, _):
            rest = step - groups * EARLY
            late = (rest // (per - EARLY)) * per + EARLY + lax.rem(rest, per - EARLY)
            q = jnp.where(rest < 0, (step // EARLY) * per + lax.rem(step, EARLY), late)
            mass_rows[0:layers] = x_ref[q, :, cs].astype(F32)
            mass = [
                mass_rows[p * ROWS : (p + 1) * ROWS] * dp_rows[p * ROWS : (p + 1) * ROWS]
                for p in range(pieces)
            ]
            moved, top = remap(mass)
            kept = jnp.zeros((ROWS, LANES), F32)
            for p, m in enumerate(moved):
                m = jnp.maximum(m, 0.0)
                kept = kept + m
                positive[q, p * ROWS : (p + 1) * ROWS, cs] = m * inverse[p]
            before = top[layers % ROWS : layers % ROWS + 1]
            part[0, pl.ds(q, 1), :] += before * area
            part[1, pl.ds(q, 1), :] += jnp.sum(kept, axis=0, keepdims=True) * area

            @pl.when(rest == 0)
            def _():
                @pl.when(block == 0)
                def _():
                    pl.semaphore_wait(barrier, devices - 1)

                for copy in early_copies(block, cs):
                    copy.start()

            return 0

        return lax.fori_loop(0, tracers, tracer, 0)

    lax.fori_loop(0, columns // LANES, column_block, 0)

    t_row = lax.broadcasted_iota(jnp.int32, (tracers, LANES), 0)
    t_lane = lax.broadcasted_iota(jnp.int32, (tracers, LANES), 1)

    def to_row(values, shift):
        return jnp.sum(jnp.where(t_row == t_lane + shift, values, 0.0), axis=0, keepdims=True)

    def to_column(values):
        return jnp.sum(jnp.where(t_row == t_lane, values, 0.0), axis=1, keepdims=True)

    packed[...] = jnp.zeros_like(packed)
    for kind in range(2):
        packed[kind : kind + 1] = to_row(jnp.sum(part[kind], axis=1, keepdims=True), 0)
    arrived[pl.ds(me, 1)] = packed[...][None]
    sums = []
    for step in range(1, devices):
        peer = lax.rem(me + step, devices)
        copy = pltpu.make_async_remote_copy(
            src_ref=packed, dst_ref=arrived.at[me], send_sem=sum_send.at[step - 1], recv_sem=sum_recv.at[step - 1],
            device_id=(peer // groups, lax.rem(peer, groups)), device_id_type=MESH,
        )
        copy.start()
        sums.append(copy)
    for copy in sums:
        copy.wait()
    total = jnp.sum(arrived[...], axis=0) * norm
    before = to_column(total[0:1])
    after = to_column(total[1:2])
    ratio[...] = jnp.broadcast_to(before / after, (tracers, LANES))
    burden_ref[...] = to_row(before, g_id * per)[:, 0:per]

    def place(h):
        return pl.ds(pl.multiple_of(h * columns, LANES), columns)

    def scaled(values, t):
        scale = jnp.tile(ratio[pl.ds(t, 1), :], (1, columns // LANES))
        return (values * scale).astype(jnp.bfloat16)

    copies = []
    for q in range(EARLY, per):
        for k in order:
            h = jnp.bitwise_xor(g_id, k)
            stage[h, q] = scaled(positive[h * per + q], h * per + q)
            copy = pltpu.make_async_remote_copy(
                src_ref=stage.at[h, q], dst_ref=out_ref.at[q, :, place(g_id)],
                send_sem=move_send.at[q, k - 1], recv_sem=move_recv.at[q, k - 1],
                device_id=(c_id, h), device_id_type=MESH,
            )
            copy.start()
            copies.append(copy)
    for q in range(per):
        stage[g_id, q] = scaled(positive[g_id * per + q], g_id * per + q)
    own = pltpu.make_async_copy(stage.at[g_id], out_ref.at[:, :, place(g_id)], own_sem.at[0])
    own.start()
    for block in range(columns // LANES):
        for copy in early_copies(block, pl.ds(block * LANES, LANES)):
            copy.wait()
    local = [own]
    for k in order:
        for e in range(EARLY):
            landed[k - 1, e] = scaled(early[k - 1, e], g_id * per + e)
        copy = pltpu.make_async_copy(
            landed.at[k - 1],
            out_ref.at[0:EARLY, :, place(jnp.bitwise_xor(g_id, k))],
            own_sem.at[k],
        )
        copy.start()
        local.append(copy)
    for copy in local + copies:
        copy.wait()


def per_device(cols, groups, tracers_src, layer_dp, cut_frac, level_bounds):
    tracers, layers, columns = tracers_src.shape
    levels = level_bounds.shape[1]
    per = tracers // groups
    padded = -(-(layers + 1) // ROWS) * ROWS
    vmem = pl.BlockSpec(memory_space=pltpu.VMEM)
    result, burden = pl.pallas_call(
        functools.partial(kernel, cols, groups),
        out_shape=(
            jax.ShapeDtypeStruct((per, levels, columns * groups), jnp.bfloat16),
            jax.ShapeDtypeStruct((1, per), F32),
        ),
        in_specs=[vmem] * 4,
        out_specs=(pl.BlockSpec(memory_space=pl.ANY), vmem),
        scratch_shapes=[
            pltpu.VMEM((tracers, levels, columns), F32),
            pltpu.VMEM((groups, per, levels, columns), jnp.bfloat16),
            pltpu.VMEM((padded, LANES), F32),
            pltpu.VMEM((padded, LANES), F32),
            pltpu.VMEM((padded // ROWS, ROWS, LANES), F32),
            pltpu.VMEM((levels, LANES), jnp.int32),
            pltpu.VMEM((levels // ROWS, ROWS, LANES), F32),
            pltpu.VMEM((2, tracers, LANES), F32),
            pltpu.VMEM((2, LANES), F32),
            pltpu.VMEM((cols * groups, 2, LANES), F32),
            pltpu.VMEM((tracers, LANES), F32),
            pltpu.VMEM((groups - 1, EARLY, levels, columns), F32),
            pltpu.VMEM((groups - 1, EARLY, levels, columns), jnp.bfloat16),
            pltpu.SemaphoreType.DMA((cols * groups - 1,)),
            pltpu.SemaphoreType.DMA((cols * groups - 1,)),
            pltpu.SemaphoreType.DMA((per, groups - 1)),
            pltpu.SemaphoreType.DMA((per, groups - 1)),
            pltpu.SemaphoreType.DMA((columns // LANES, EARLY, groups - 1)),
            pltpu.SemaphoreType.DMA((columns // LANES, EARLY, groups - 1)),
            pltpu.SemaphoreType.DMA((groups,)),
        ],
        compiler_params=pltpu.CompilerParams(
            collective_id=0, has_side_effects=True, vmem_limit_bytes=60 * 1024 * 1024
        ),
        name="remap_fix_exchange",
    )(tracers_src, layer_dp, cut_frac, level_bounds)
    return result, burden.reshape(per)


def solution(mesh):
    spread = ("cols", "trc")
    in_specs = (P(None, None, spread), P(None, spread), P(None, spread), P(None, None, spread))
    out_specs = (P("trc", None, "cols"), P("trc"))
    return jax.shard_map(
        functools.partial(per_device, mesh.shape["cols"], mesh.shape["trc"]),
        mesh=mesh, in_specs=in_specs, out_specs=out_specs, check_vma=False,
    )
```

```python
import functools

import jax
import jax.numpy as jnp
from jax import lax
from jax.experimental import pallas as pl
from jax.experimental.pallas import tpu as pltpu
from jax.sharding import PartitionSpec as P

MESH = pl.DeviceIdType.MESH
F32 = jnp.float32
LANES = 128
ROWS = 8
EARLY = 2
HELD = 1


def take_rows(values, rows):
    return jnp.take_along_axis(values, rows, axis=0, mode="promise_in_bounds")


def running_sum(pieces, row):
    result, carry = [], None
    last = jnp.full((ROWS, LANES), ROWS - 1, jnp.int32)
    for piece in pieces:
        for step in (1, 2, 4):
            piece = piece + jnp.where(row >= step, pltpu.roll(piece, step, 0), 0.0)
        total = take_rows(piece, last)
        result.append(piece if carry is None else piece + carry)
        carry = total if carry is None else carry + total
    return result


def edge_values(values, low, high, layers, levels):
    slack = layers - levels
    edges = []
    for piece in range(levels // ROWS):
        first = (piece * ROWS + 1) // ROWS
        final = min((piece * ROWS + ROWS + slack) // ROWS, len(values) - 1)
        picked = None
        for source in range(first, final + 1):
            here = take_rows(values[source], low[piece])
            picked = here if picked is None else jnp.where(high[piece] == source, here, picked)
        edges.append(picked)
    return edges


def differences(edges, row):
    result, before = [], jnp.zeros((ROWS, LANES), F32)
    for edge in edges:
        turned = pltpu.roll(edge, 1, 0)
        result.append(edge - jnp.where(row == 0, before, turned))
        before = turned
    return result


def kernel(
    cols, groups, x_ref, dp_ref, cut_ref, bounds_ref, out_ref, burden_ref,
    positive, stage, mass_rows, dp_rows, blend, target, inverse, part, packed, arrived, ratio,
    early, landed, sum_send, sum_recv, move_send, move_recv, early_send, early_recv, own_sem,
):
    tracers, layers, columns = x_ref.shape
    levels = bounds_ref.shape[1]
    per = tracers // groups
    devices = cols * groups
    pieces = (layers + ROWS) // ROWS
    slack = layers - levels
    c_id, g_id = lax.axis_index("cols"), lax.axis_index("trc")
    me = c_id * groups + g_id
    norm = 1.0 / (columns * devices * layers)

    barrier = pltpu.get_barrier_semaphore()
    others = [lax.rem(me + step, devices) for step in range(1, devices)]
    peers = [(other // groups, lax.rem(other, groups)) for other in others]
    for peer in peers:
        pl.semaphore_signal(barrier, inc=1, device_id=peer, device_id_type=MESH)

    row = lax.broadcasted_iota(jnp.int32, (ROWS, LANES), 0)
    lane = lax.broadcasted_iota(jnp.int32, (1, LANES), 1)
    part[...] = jnp.zeros_like(part)
    mass_rows[...] = jnp.zeros_like(mass_rows)
    dp_rows[...] = jnp.zeros_like(dp_rows)

    order = sorted(range(1, groups), reverse=True)

    def early_copies(block, cs):
        copies = []
        for e in range(EARLY):
            for k in order:
                h = jnp.bitwise_xor(g_id, k)
                copies.append(pltpu.make_async_remote_copy(
                    src_ref=positive.at[h * per + e, :, cs], dst_ref=early.at[k - 1, e, :, cs],
                    send_sem=early_send.at[block, e, k - 1], recv_sem=early_recv.at[block, e, k - 1],
                    device_id=(c_id, h), device_id_type=MESH,
                ))
        return copies

    def column_block(block, _):
        offset = pl.multiple_of(block * LANES, LANES)
        cs = pl.ds(offset, LANES)
        target[0 : levels - 1] = bounds_ref[0, 1:, cs]
        target[levels - 1 : levels] = jnp.full((1, LANES), layers, jnp.int32)
        dp_rows[0:layers] = dp_ref[:, cs]
        for piece in range(pieces):
            first = max(1, piece * ROWS - slack)
            final = min(levels - 1, piece * ROWS + ROWS - 1)
            weight = jnp.full((ROWS, LANES), -1.0, F32)
            for j in range(first, final + 1):
                found = target[j - 1 : j] == row + piece * ROWS
                weight = jnp.where(found, cut_ref[j - 1 : j, cs] - 1.0, weight)
            blend[piece] = weight
        bounds = [target[p * ROWS : (p + 1) * ROWS] for p in range(levels // ROWS)]
        low = [jnp.bitwise_and(b, ROWS - 1) for b in bounds]
        high = [lax.shift_right_logical(b, 3) for b in bounds]

        def remap(mass):
            sums = running_sum(mass, row)
            values = [s + blend[p] * m for p, (s, m) in enumerate(zip(sums, mass))]
            edges = edge_values(values, low, high, layers, levels)
            return differences(edges, row), values[-1]

        thickness, _ = remap([dp_rows[p * ROWS : (p + 1) * ROWS] for p in range(pieces)])
        for p, t in enumerate(thickness):
            inverse[p] = 1.0 / t
        area = 1.0 + 2.0 * (lane + offset + me * columns).astype(F32) / (columns * devices)

        def tracer(step, _):
            rest = step - groups * EARLY
            late = (rest // (per - EARLY)) * per + EARLY + lax.rem(rest, per - EARLY)
            q = jnp.where(rest < 0, (step // EARLY) * per + lax.rem(step, EARLY), late)
            mass_rows[0:layers] = x_ref[q, :, cs].astype(F32)
            mass = [
                mass_rows[p * ROWS : (p + 1) * ROWS] * dp_rows[p * ROWS : (p + 1) * ROWS]
                for p in range(pieces)
            ]
            moved, top = remap(mass)
            kept = jnp.zeros((ROWS, LANES), F32)
            for p, m in enumerate(moved):
                m = jnp.maximum(m, 0.0)
                kept = kept + m
                positive[q, p * ROWS : (p + 1) * ROWS, cs] = m * inverse[p]
            before = top[layers % ROWS : layers % ROWS + 1]
            part[0, pl.ds(q, 1), :] += before * area
            part[1, pl.ds(q, 1), :] += jnp.sum(kept, axis=0, keepdims=True) * area

            @pl.when(rest == 0)
            def _():
                @pl.when(block == 0)
                def _():
                    pl.semaphore_wait(barrier, devices - 1)

                @pl.when(block < columns // LANES - HELD)
                def _():
                    for copy in early_copies(block, cs):
                        copy.start()

            return 0

        return lax.fori_loop(0, tracers, tracer, 0)

    lax.fori_loop(0, columns // LANES, column_block, 0)

    t_row = lax.broadcasted_iota(jnp.int32, (tracers, LANES), 0)
    t_lane = lax.broadcasted_iota(jnp.int32, (tracers, LANES), 1)

    def to_row(values, shift):
        return jnp.sum(jnp.where(t_row == t_lane + shift, values, 0.0), axis=0, keepdims=True)

    def to_column(values):
        return jnp.sum(jnp.where(t_row == t_lane, values, 0.0), axis=1, keepdims=True)


    def share(values, source, slots, slot, peers, send_sem, recv_sem):
        source[...] = values
        slots[pl.ds(slot, 1)] = values[None]
        sums = []
        for i, peer in enumerate(peers):
            copy = pltpu.make_async_remote_copy(
                src_ref=source, dst_ref=slots.at[slot], send_sem=send_sem.at[i],
                recv_sem=recv_sem.at[i], device_id=peer, device_id_type=MESH,
            )
            copy.start()
            sums.append(copy)
        for block in range(columns // LANES - HELD, columns // LANES):
            for copy in early_copies(block, pl.ds(block * LANES, LANES)):
                copy.start()
        for copy in sums:
            copy.wait()
        return jnp.sum(slots[...], axis=0)

    mine = jnp.concatenate(
        [to_row(jnp.sum(part[kind], axis=1, keepdims=True), 0) for kind in range(2)], axis=0
    )
    total = share(mine, packed, arrived, me, peers, sum_send, sum_recv) * norm
    before = to_column(total[0:1])
    after = to_column(total[1:2])
    ratio[...] = jnp.broadcast_to(before / after, (tracers, LANES))
    burden_ref[...] = to_row(before, g_id * per)[:, 0:per]

    def place(h):
        return pl.ds(pl.multiple_of(h * columns, LANES), columns)

    def scaled(values, t):
        scale = jnp.tile(ratio[pl.ds(t, 1), :], (1, columns // LANES))
        return (values * scale).astype(jnp.bfloat16)

    copies = []
    for q in range(EARLY, per):
        for k in order:
            h = jnp.bitwise_xor(g_id, k)
            stage[h, q] = scaled(positive[h * per + q], h * per + q)
            copy = pltpu.make_async_remote_copy(
                src_ref=stage.at[h, q], dst_ref=out_ref.at[q, :, place(g_id)],
                send_sem=move_send.at[q, k - 1], recv_sem=move_recv.at[q, k - 1],
                device_id=(c_id, h), device_id_type=MESH,
            )
            copy.start()
            copies.append(copy)
    for q in range(per):
        stage[g_id, q] = scaled(positive[g_id * per + q], g_id * per + q)
    own = pltpu.make_async_copy(stage.at[g_id], out_ref.at[:, :, place(g_id)], own_sem.at[0])
    own.start()
    for block in range(columns // LANES):
        for copy in early_copies(block, pl.ds(block * LANES, LANES)):
            copy.wait()
    local = [own]
    for k in order:
        for e in range(EARLY):
            landed[k - 1, e] = scaled(early[k - 1, e], g_id * per + e)
        copy = pltpu.make_async_copy(
            landed.at[k - 1],
            out_ref.at[0:EARLY, :, place(jnp.bitwise_xor(g_id, k))],
            own_sem.at[k],
        )
        copy.start()
        local.append(copy)
    for copy in local + copies:
        copy.wait()


def per_device(cols, groups, tracers_src, layer_dp, cut_frac, level_bounds):
    tracers, layers, columns = tracers_src.shape
    levels = level_bounds.shape[1]
    per = tracers // groups
    padded = -(-(layers + 1) // ROWS) * ROWS
    vmem = pl.BlockSpec(memory_space=pltpu.VMEM)
    result, burden = pl.pallas_call(
        functools.partial(kernel, cols, groups),
        out_shape=(
            jax.ShapeDtypeStruct((per, levels, columns * groups), jnp.bfloat16),
            jax.ShapeDtypeStruct((1, per), F32),
        ),
        in_specs=[vmem] * 4,
        out_specs=(pl.BlockSpec(memory_space=pl.ANY), vmem),
        scratch_shapes=[
            pltpu.VMEM((tracers, levels, columns), F32),
            pltpu.VMEM((groups, per, levels, columns), jnp.bfloat16),
            pltpu.VMEM((padded, LANES), F32),
            pltpu.VMEM((padded, LANES), F32),
            pltpu.VMEM((padded // ROWS, ROWS, LANES), F32),
            pltpu.VMEM((levels, LANES), jnp.int32),
            pltpu.VMEM((levels // ROWS, ROWS, LANES), F32),
            pltpu.VMEM((2, tracers, LANES), F32),
            pltpu.VMEM((2, LANES), F32),
            pltpu.VMEM((cols * groups, 2, LANES), F32),
            pltpu.VMEM((tracers, LANES), F32),
            pltpu.VMEM((groups - 1, EARLY, levels, columns), F32),
            pltpu.VMEM((groups - 1, EARLY, levels, columns), jnp.bfloat16),
            pltpu.SemaphoreType.DMA((cols * groups - 1,)),
            pltpu.SemaphoreType.DMA((cols * groups - 1,)),
            pltpu.SemaphoreType.DMA((per, groups - 1)),
            pltpu.SemaphoreType.DMA((per, groups - 1)),
            pltpu.SemaphoreType.DMA((columns // LANES, EARLY, groups - 1)),
            pltpu.SemaphoreType.DMA((columns // LANES, EARLY, groups - 1)),
            pltpu.SemaphoreType.DMA((groups,)),
        ],
        compiler_params=pltpu.CompilerParams(
            collective_id=0, has_side_effects=True, vmem_limit_bytes=60 * 1024 * 1024
        ),
        name="remap_fix_exchange",
    )(tracers_src, layer_dp, cut_frac, level_bounds)
    return result, burden.reshape(per)


def solution(mesh):
    spread = ("cols", "trc")
    in_specs = (P(None, None, spread), P(None, spread), P(None, spread), P(None, None, spread))
    out_specs = (P("trc", None, "cols"), P("trc"))
    return jax.shard_map(
        functools.partial(per_device, mesh.shape["cols"], mesh.shape["trc"]),
        mesh=mesh, in_specs=in_specs, out_specs=out_specs, check_vma=False,
    )
```
